32 devices in a mesh: grp: 4 (over y, x), slab: 8 (over z, core).
Axes of the slice: x: 2, y: 2, z: 4, core: 2. Of those that a mesh axis runs over, the one named last changes fastest.
Arguments:
- state: float32 [4, 2, 256, 128, 256], P(None, None, 'grp', 'slab'), may hold values from -5.6 to 5.6
- kz_group: int32 [256], replicated, may hold values from 0 to 7, as said below
- cutoffs: int32 [3], replicated, may hold values from 28 to 32
- damping: float32 [8], replicated, may hold values from 0.005 to 0.5
- power: float32 [8], replicated, may hold values from 0.2 to 4
Outputs:
- new_state: float32 [4, 2, 256, 128, 256], P(None, None, 'grp', 'slab')
The draws below stay inside these ranges and needn't reach their ends.
Inputs may be any that keep to these rules, and one draw needn't show every extreme that they name: `kz_group`: each of the 8 groups holds exactly 32 indices.
All inputs are finite; a program needn't handle non-finite values.
Results may differ from the reference program's by a relative error of at most 0.00005.
Values sent between devices are 32-bit elements; how exact they have to be, the bound alone decides.
A program may use at most 192 MiB of HBM per device.

```python
import math
import jax
import jax.numpy as jnp
from jax import lax

NX = 256
NY = 256
NZ = 256
GROUPS = 8
KX = 128
GMODES = 32


def draw_state(key, part):
    noise = jnp.clip(jax.random.normal(key, (4, 2, NZ, KX, NY), jnp.float32), -4.0, 4.0)
    rate = 0.7
    mixing = 0.6
    decay = jnp.exp(-rate * jnp.arange(KX, dtype=jnp.float32) / KX)[None, None, None, :, None]
    noise = noise * decay
    buoyant = mixing * noise[2] + 0.8 * noise[3]
    return jnp.concatenate([noise[:3], buoyant[None]], axis=0)


def draw_kz_group(key, part):
    ordering = jax.random.permutation(key, NZ)
    return (ordering // (NZ // GROUPS)).astype(jnp.int32)


def setup_inputs(seed: int = 0) -> dict:
    seeds = jax.random.split(jax.random.key(seed), 6)
    return {
        "state": draw_state(jax.random.fold_in(seeds[5], 71), 0),
        "kz_group": draw_kz_group(jax.random.fold_in(seeds[5], 71), 0),
        "cutoffs": jax.random.randint(seeds[2], (3,), 28, 33).astype(jnp.int32),
        "damping": jnp.clip(jnp.exp(jax.random.uniform(seeds[3], (GROUPS,), jnp.float32, math.log(0.005), math.log(0.5))), 0.005, 0.5),
        "power": jnp.clip(jnp.exp(jax.random.uniform(seeds[4], (GROUPS,), jnp.float32, math.log(0.2), math.log(4.0))), 0.2, 4.0),
    }


TIME_STEP = 0.25
CORIOLIS = 1.0
BRUNT_SQUARED = 2.0
EPSILON = 1e-06

def signed(index, length):
    return jnp.where(index < length // 2, index, index - length)

def to_grid(field, slot_mode, weights):
    padded = jnp.zeros((NZ, NX, NY), field.dtype)
    padded = padded.at[slot_mode, :KX, :].set(field * weights[None, :, None])
    return jnp.real(jnp.fft.ifftn(padded)) * math.sqrt(NX * NY * NZ)

def to_spectral(values, slot_mode):
    full = jnp.fft.fftn(values) / math.sqrt(NX * NY * NZ)
    return full[slot_mode][:, :KX, :]

def squared(entries):
    return jnp.real(entries) ** 2 + jnp.imag(entries) ** 2

def reference(state, kz_group, cutoffs, damping, power):
    float_type = state.dtype
    slot_mode = jnp.argsort(kz_group, stable=True).astype(jnp.int32)
    mode_z = signed(slot_mode, NZ)
    mode_x = jnp.arange(KX, dtype=jnp.int32)
    mode_y = signed(jnp.arange(NY, dtype=jnp.int32), NY)
    wave_z = (2.0 * math.pi / NZ * mode_z.astype(float_type))[:, None, None]
    wave_x = (2.0 * math.pi / NX * mode_x.astype(float_type))[None, :, None]
    wave_y = (2.0 * math.pi / NY * mode_y.astype(float_type))[None, None, :]
    spectra = state[:, 0] + 1j * state[:, 1]
    flow_x, flow_y, flow_z, buoyant = (spectra[0], spectra[1], spectra[2], spectra[3])
    swirl_x = 1j * (wave_y * flow_z - wave_z * flow_y)
    swirl_y = 1j * (wave_z * flow_x - wave_x * flow_z)
    swirl_z = 1j * (wave_x * flow_y - wave_y * flow_x)
    weights = jnp.where(mode_x == 0, 1.0, 2.0).astype(float_type)
    grids = [to_grid(field, slot_mode, weights) for field in (flow_x, flow_y, flow_z, buoyant, swirl_x, swirl_y, swirl_z)]
    grid_u, grid_v, grid_w, grid_b, grid_ox, grid_oy, grid_oz = grids
    products = [grid_v * grid_oz - grid_w * grid_oy, grid_w * grid_ox - grid_u * grid_oz, grid_u * grid_oy - grid_v * grid_ox, grid_u * grid_b, grid_v * grid_b, grid_w * grid_b]
    hats = [to_spectral(product, slot_mode) for product in products]
    kept = ((96 * jnp.abs(mode_z) <= cutoffs[2] * NZ)[:, None, None] & (96 * mode_x <= cutoffs[0] * NX)[None, :, None] & (96 * jnp.abs(mode_y) <= cutoffs[1] * NY)[None, None, :]).astype(float_type)
    moment_x, moment_y, moment_z = (kept * hats[0], kept * hats[1], kept * hats[2])
    source_b = -1j * kept * (wave_x * hats[3] + wave_y * hats[4] + wave_z * hats[5])
    cell_flux = jnp.real(flow_z) * jnp.real(buoyant) + jnp.imag(flow_z) * jnp.imag(buoyant)
    cell_energy = 0.5 * (squared(flow_x) + squared(flow_y) + squared(flow_z) + squared(buoyant) / BRUNT_SQUARED)
    modes_total = GMODES * KX * NY
    flux_mean = lax.optimization_barrier(jnp.sum(cell_flux.reshape(GROUPS, -1), axis=1)) / modes_total
    energy_mean = lax.optimization_barrier(jnp.sum(cell_energy.reshape(GROUPS, -1), axis=1)) / modes_total
    forcing = (power - flux_mean) / (2.0 * (energy_mean + EPSILON))
    forcing_slot = jnp.repeat(forcing, GMODES)[:, None, None]
    damping_slot = jnp.repeat(damping, GMODES)[:, None, None]
    right_x = flow_x + TIME_STEP * (moment_x + forcing_slot * flow_x)
    right_y = flow_y + TIME_STEP * (moment_y + forcing_slot * flow_y)
    right_z = flow_z + TIME_STEP * (moment_z + forcing_slot * flow_z)
    right_b = buoyant + TIME_STEP * source_b
    wave_sq = wave_x * wave_x + wave_y * wave_y + wave_z * wave_z
    implicit = 1.0 + TIME_STEP * damping_slot * wave_sq
    rotation = TIME_STEP * CORIOLIS
    first_den = implicit * implicit + rotation * rotation
    second_den = implicit * implicit + TIME_STEP * TIME_STEP * BRUNT_SQUARED
    new_x = (implicit * right_x + rotation * right_y) / first_den
    new_y = (implicit * right_y - rotation * right_x) / first_den
    new_z = (implicit * right_z + TIME_STEP * right_b) / second_den
    new_b = (implicit * right_b - TIME_STEP * BRUNT_SQUARED * right_z) / second_den
    inverse_sq = 1.0 / (wave_sq + (wave_sq == 0).astype(float_type))
    inner = (wave_x * new_x + wave_y * new_y + wave_z * new_z) * inverse_sq
    new_x = new_x - wave_x * inner
    new_y = new_y - wave_y * inner
    new_z = new_z - wave_z * inner
    return jnp.stack([jnp.stack([jnp.real(updated), jnp.imag(updated)]) for updated in (new_x, new_y, new_z, new_b)]).astype(float_type)
```

```python
import math

import jax
import jax.numpy as jnp
from jax import lax
from jax.sharding import PartitionSpec as P

PRECISE = lax.Precision.HIGH
TWO_PI = 6.283185307179586
TIME_STEP = 0.25
CORIOLIS = 1.0
BRUNT_SQUARED = 2.0
EPSILON = 1e-06


def signed(index, length):
    return jnp.where(index < length // 2, index, index - length)


def angles(modes, points, length):
    phase = modes[:, None] * points[None, :] % length
    theta = phase.astype(jnp.float32) * (TWO_PI / length)
    return (jnp.cos(theta), jnp.sin(theta))


def times_i(entries):
    return jnp.stack([-entries[1], entries[0]])


def mul(pattern, left, right):
    return jnp.einsum(pattern, left, right, precision=PRECISE)


def exchange(pieces, axis):
    shape = pieces.shape
    flat = pieces.reshape(shape[0], -1, shape[-2] * shape[-1])
    return lax.all_to_all(flat, axis, split_axis=0, concat_axis=0, tiled=True).reshape(shape)


def shards(state, kz_group, cutoffs, damping, power):
    grp_count = lax.axis_size("grp")
    slab_count = lax.axis_size("slab")
    grp_index = lax.axis_index("grp")
    slab_index = lax.axis_index("slab")
    slots_here = state.shape[2]
    cols_here = state.shape[3]
    NY = state.shape[4]
    NZ = slots_here * grp_count
    KX = cols_here * slab_count
    NX = 2 * KX
    GROUPS = damping.shape[0]
    GMODES = NZ // GROUPS
    rows_here = NY // grp_count
    planes_here = NZ // slab_count
    groups_here = GROUPS // grp_count
    normalizer = 1.0 / math.sqrt(NX * NY * NZ)
    slot_mode = jnp.argsort(kz_group, stable=True)
    local_mode = lax.dynamic_slice_in_dim(slot_mode, grp_index * slots_here, slots_here)
    mode_z = signed(local_mode, NZ)
    mode_x = slab_index * cols_here + jnp.arange(cols_here, dtype=jnp.int32)
    mode_y = signed(jnp.arange(NY, dtype=jnp.int32), NY)
    wave_z = (TWO_PI / NZ * mode_z.astype(jnp.float32))[:, None, None]
    wave_x = (TWO_PI / NX * mode_x.astype(jnp.float32))[None, :, None]
    wave_y = (TWO_PI / NY * mode_y.astype(jnp.float32))[None, None, :]
    flow_x, flow_y, flow_z, buoyant = (state[0], state[1], state[2], state[3])

    real_part = state[:, 0]
    imag_part = state[:, 1]
    cell_flux = real_part[2] * real_part[3] + imag_part[2] * imag_part[3]
    cell_energy = 0.5 * (
        jnp.sum(real_part[:3] ** 2 + imag_part[:3] ** 2, axis=0)
        + (real_part[3] ** 2 + imag_part[3] ** 2) / BRUNT_SQUARED
    )
    partial_value = jnp.stack(
        [jnp.sum(cell_flux, axis=(1, 2)), jnp.sum(cell_energy, axis=(1, 2))], axis=1
    )
    partial_value = jnp.sum(partial_value.reshape(groups_here, GMODES, 2), axis=1)
    totals = lax.psum(partial_value, "slab")
    means = totals / (GMODES * KX * NY)

    points_y = jnp.arange(NY, dtype=jnp.int32)
    points_z = jnp.arange(NZ, dtype=jnp.int32)
    points_x = jnp.arange(NX, dtype=jnp.int32)
    cosine_y, sine_y = angles(points_y, points_y, NY)
    from_real = jnp.stack([cosine_y, sine_y], axis=1)
    from_imag = jnp.stack([-sine_y, cosine_y], axis=1)
    column = wave_y.reshape(NY, 1, 1)
    shape_y = (NY, 2, grp_count, rows_here)
    spread = "fsxm,mdgy->gfdsxy"
    main = mul(spread, real_part, from_real.reshape(shape_y)) + mul(
        spread, imag_part, from_imag.reshape(shape_y)
    )
    slope = mul(spread, real_part[::2][:2], (column * from_imag).reshape(shape_y)) - mul(
        spread, imag_part[::2][:2], (column * from_real).reshape(shape_y)
    )
    pieces = exchange(jnp.concatenate([main, slope], axis=1), "grp")

    all_z = (TWO_PI / NZ * signed(slot_mode, NZ).astype(jnp.float32)).reshape(
        grp_count, slots_here, 1, 1
    )
    real_in, imag_in = (pieces[:, :, 0], pieces[:, :, 1])
    ru, rv, rw, rb, ruy, rwy = (real_in[:, k] for k in range(6))
    iu, iv, iw, ib, iuy, iwy = (imag_in[:, k] for k in range(6))
    reals = [ru, rv, rw, rb, rwy + all_z * iv, wave_x * iw - all_z * iu, -wave_x * iv - ruy]
    imags = [iu, iv, iw, ib, iwy - all_z * rv, all_z * ru - wave_x * rw, wave_x * rv - iuy]
    width = cols_here * rows_here
    reals = jnp.stack([r.reshape(NZ, width) for r in reals])
    imags = jnp.stack([r.reshape(NZ, width) for r in imags])
    cosine_z, sine_z = angles(slot_mode, points_z, NZ)
    shape_z = (NZ, 2, slab_count, planes_here)
    spread = "fsn,sdlz->lfdzn"
    grid_z = mul(spread, reals, jnp.stack([cosine_z, sine_z], axis=1).reshape(shape_z)) + mul(
        spread, imags, jnp.stack([-sine_z, cosine_z], axis=1).reshape(shape_z)
    )
    grid_z = grid_z.reshape(slab_count, 7, 2, planes_here, cols_here, rows_here)
    pieces = exchange(grid_z, "slab")

    weights = jnp.where(jnp.arange(KX) == 0, 1.0, 2.0).astype(jnp.float32) * normalizer
    cosine_x, sine_x = angles(jnp.arange(KX, dtype=jnp.int32), points_x, NX)
    shape_x = (2, slab_count, cols_here, NX)
    table_x = jnp.stack([cosine_x * weights[:, None], -sine_x * weights[:, None]]).reshape(shape_x)
    lines = pieces.transpose(1, 3, 5, 2, 0, 4).reshape(7, planes_here, rows_here, 2 * KX)
    grid = mul("fzyk,kn->fzyn", lines, table_x.reshape(2 * KX, NX))
    gu, gv, gw, gb, gox, goy, goz = (grid[k] for k in range(7))
    products = jnp.stack(
        [gv * goz - gw * goy, gw * gox - gu * goz, gu * goy - gv * gox, gu * gb, gv * gb, gw * gb]
    )
    table_b = jnp.stack([cosine_x * normalizer, -sine_x * normalizer]).reshape(2 * KX, NX)
    sectioned = mul("fzyn,kn->fzyk", products, table_b)
    sectioned = sectioned.reshape(6, planes_here, rows_here, 2, slab_count, cols_here)
    pieces = exchange(sectioned.transpose(4, 0, 3, 1, 5, 2), "slab")

    reals = pieces[:, :, 0].reshape(slab_count, 6, planes_here, width)
    imags = pieces[:, :, 1].reshape(slab_count, 6, planes_here, width)
    shape_z = (slab_count, planes_here, 2, grp_count, slots_here)
    cosine_z, sine_z = (cosine_z.T, sine_z.T)
    spread = "lfzn,lzdgs->dfgsn"
    back_z = mul(spread, reals, jnp.stack([cosine_z, -sine_z], axis=1).reshape(shape_z)) + mul(
        spread, imags, jnp.stack([sine_z, cosine_z], axis=1).reshape(shape_z)
    )
    back_z = back_z.reshape(2, 6, grp_count, slots_here, cols_here, rows_here)
    moved = wave_x * back_z[:, 3] + all_z * back_z[:, 5]
    chosen = [back_z[:, 0], back_z[:, 1], back_z[:, 2], moved, back_z[:, 4]]
    sent = jnp.stack([c.transpose(1, 0, 2, 3, 4) for c in chosen], axis=1)
    pieces = exchange(sent, "grp")

    lines = pieces.transpose(1, 2, 3, 4, 0, 5).reshape(5, 2, slots_here, cols_here, NY)
    table_r = jnp.stack([cosine_y, -sine_y], axis=1)
    table_i = jnp.stack([sine_y, cosine_y], axis=1)
    spread = "fsxy,ydm->fdsxm"
    tendency = mul(spread, lines[:, 0], table_r) + mul(spread, lines[:, 1], table_i)

    kept = (
        (96 * jnp.abs(mode_z) <= cutoffs[2] * NZ)[:, None, None]
        & (96 * mode_x <= cutoffs[0] * NX)[None, :, None]
        & (96 * jnp.abs(mode_y) <= cutoffs[1] * NY)[None, None, :]
    ).astype(jnp.float32)
    moment_x, moment_y, moment_z = (tendency[0] * kept, tendency[1] * kept, tendency[2] * kept)
    divergence = tendency[3] + wave_y * tendency[4]
    source_b = jnp.stack([divergence[1], -divergence[0]]) * kept
    power_here = lax.dynamic_slice_in_dim(power, grp_index * groups_here, groups_here)
    damping_here = lax.dynamic_slice_in_dim(damping, grp_index * groups_here, groups_here)
    forcing = (power_here - means[:, 0]) / (2.0 * (means[:, 1] + EPSILON))
    forcing_slot = jnp.repeat(forcing, GMODES)[:, None, None]
    damping_slot = jnp.repeat(damping_here, GMODES)[:, None, None]
    right_x = flow_x + TIME_STEP * (moment_x + forcing_slot * flow_x)
    right_y = flow_y + TIME_STEP * (moment_y + forcing_slot * flow_y)
    right_z = flow_z + TIME_STEP * (moment_z + forcing_slot * flow_z)
    right_b = buoyant + TIME_STEP * source_b
    wave_sq = wave_x * wave_x + wave_y * wave_y + wave_z * wave_z
    implicit = 1.0 + TIME_STEP * damping_slot * wave_sq
    rotation = TIME_STEP * CORIOLIS
    first_den = implicit * implicit + rotation * rotation
    second_den = implicit * implicit + TIME_STEP * TIME_STEP * BRUNT_SQUARED
    new_x = (implicit * right_x + rotation * right_y) / first_den
    new_y = (implicit * right_y - rotation * right_x) / first_den
    new_z = (implicit * right_z + TIME_STEP * right_b) / second_den
    new_b = (implicit * right_b - TIME_STEP * BRUNT_SQUARED * right_z) / second_den
    inverse_sq = 1.0 / (wave_sq + (wave_sq == 0).astype(jnp.float32))
    inner = (wave_x * new_x + wave_y * new_y + wave_z * new_z) * inverse_sq
    new_x = new_x - wave_x * inner
    new_y = new_y - wave_y * inner
    new_z = new_z - wave_z * inner
    return jnp.stack([new_x, new_y, new_z, new_b])


def solution(mesh):
    return jax.shard_map(
        shards,
        mesh=mesh,
        in_specs=(P(None, None, "grp", "slab", None), P(), P(), P(), P()),
        out_specs=P(None, None, "grp", "slab", None),
        check_vma=False,
    )
```
